32 devices in a mesh: gx: 4 (over y, core), gy: 4 (over z), gz: 2 (over x).
Axes of the slice: x: 2, y: 2, z: 4, core: 2. Of those that a mesh axis runs over, the one named last changes fastest.
Arguments:
- spin_vectors: float32 [2, 3, 32, 32, 256], P(None, None, 'gx', 'gy', 'gz'), may hold values from -1 to 1, as said below
- displacement: float32 [2, 3, 32, 32, 256], P(None, None, 'gx', 'gy', 'gz'), may hold values from -0.15 to 0.15
- occupied: int32 [2, 32, 32, 256], P(None, 'gx', 'gy', 'gz'), may hold values 0 or 1
- applied_field: float32 [3], replicated, may hold values from -4 to 4
Outputs:
- new_spins: float32 [2, 3, 32, 32, 256], P(None, None, 'gx', 'gy', 'gz')
- forces: float32 [2, 3, 32, 32, 256], P(None, None, 'gx', 'gy', 'gz')
The draws below stay inside these ranges and needn't reach their ends.
Inputs may be any that keep to these rules, and one draw needn't show every extreme that they name: `occupied`: 1 where a lattice site holds an atom, 0 at a vacancy. `spin_vectors`: every spin vector has unit length.
All inputs are finite; a program needn't handle non-finite values. No bound on the sum of `occupied` on one device may be relied on, other than what follows from the above.
Results may differ from the reference program's by a relative error of at most 0.0001.
Values sent between devices are 32-bit elements; how exact they have to be, the bound alone decides.
A program may use at most 64 MiB of HBM per device.

```python
import math
import jax
import jax.numpy as jnp
from jax import lax

CX = 8
CY = 8
NX = 32
NY = 32
NZ = 256


def draw_spin_vectors(key, part):
    height_key, azimuth_key = jax.random.split(jax.random.fold_in(key, 11))
    extent = (2, NX, NY, NZ)
    height = jax.random.uniform(height_key, extent, jnp.float32, -1.0, 1.0)
    azimuth = jax.random.uniform(azimuth_key, extent, jnp.float32, -math.pi, math.pi)
    radius = jnp.sqrt(jnp.maximum(1.0 - height * height, 0.0))
    return jnp.stack([radius * jnp.cos(azimuth), radius * jnp.sin(azimuth), height], axis=1)


def with_ends(values, rng, low, largest):
    shape = values.shape
    index_at = [jax.random.randint(jax.random.fold_in(rng, axis), (), 0, shape[axis]) for axis in range(len(shape))]
    values = values.at[tuple(index_at)].set(low)
    longest = shape.index(max(shape))
    index_at[longest] = (index_at[longest] + 1) % shape[longest]
    return values.at[tuple(index_at)].set(largest)


def block_scale(key, dims, cuts, smallest, top_value):
    def one(axis_at, blocks):
        heights = jax.random.uniform(jax.random.fold_in(jax.random.fold_in(key, 6), axis_at), (blocks,), jnp.float32, smallest / len(cuts), top_value / len(cuts))
        return jnp.repeat(jnp.exp(heights), dims[axis_at] // blocks).reshape((-1,) + (1,) * (len(dims) - axis_at - 1))

    level = one(*cuts[0])
    for cut in cuts[1:]:
        level = level * one(*cut)
    return level


def centred(key, shape, width, limit, shards=(), kind=jnp.bfloat16):
    entries = jax.random.normal(key, shape, jnp.float32) * width
    if len(shards) > 0:
        entries = block_scale(key, shape, shards, -0.22, 0.18) * entries
    return jnp.clip(entries, min=-limit, max=limit).astype(kind)


def setup_inputs(seed: int = 0) -> dict:
    key_list = jax.random.split(jax.random.key(seed), 5)
    spin_vectors = draw_spin_vectors(jax.random.fold_in(key_list[4], 71), 0)
    displacement = centred(key_list[1], (2, 3, NX, NY, NZ), 0.04, 0.15, ((2, 4), (3, 4), (4, 2)), jnp.float32)
    occupied = with_ends((jax.random.randint(key_list[2], (2, NX, NY, NZ), 0, 16) < 15).astype(jnp.int32), jax.random.fold_in(key_list[2], 1), 0, 1)
    applied_field = centred(key_list[3], (3,), 1.0, 4.0, (), jnp.float32)
    return {"spin_vectors": spin_vectors, "displacement": displacement, "occupied": occupied, "applied_field": applied_field}


step_time = 0.6
exchange_scale = 0.35
exchange_decay = 4.0
pair_scale = 0.5
pair_decay = 6.0
density_decay = 3.0
bond_length = 0.8660254037844386
corner_offsets = [(a, b, c) for a in (0, 1) for b in (0, 1) for c in (0, 1)]

def roll_cells(values, offset, sign):
    return jnp.roll(values, tuple((sign * o for o in offset)), axis=(-3, -2, -1))

def cross_product(left, right):
    return jnp.stack([left[1] * right[2] - left[2] * right[1], left[2] * right[0] - left[0] * right[2], left[0] * right[1] - left[1] * right[0]])

def rotate(spin_state, torque, fraction):
    rotation = 0.5 * fraction * torque
    first_turn = cross_product(rotation, spin_state)
    second_turn = cross_product(rotation, first_turn)
    factor = 2.0 / (1.0 + lax.optimization_barrier(jnp.sum(rotation * rotation, axis=0)))
    return spin_state + factor * (first_turn + second_turn)

def geometry(displacement, occupancy, offset):
    partner = roll_cells(displacement[1], offset, 1)
    vector = jnp.stack([0.5 - offset[i] + partner[i] - displacement[0][i] for i in range(3)])
    length = jnp.sqrt(lax.optimization_barrier(jnp.sum(vector * vector, axis=0)))
    weight = occupancy[0] * roll_cells(occupancy[1], offset, 1)
    return (vector, length, weight)

def reference(spin_vectors, displacement, occupied, applied_field):
    occupancy = occupied.astype(jnp.float32)
    external = applied_field[:, None, None, None]
    cell_x = jnp.arange(spin_vectors.shape[2])[:, None, None]
    cell_y = jnp.arange(spin_vectors.shape[3])[None, :, None]
    x_half = cell_x // (CX // 2) % 2
    y_half = cell_y // (CY // 2) % 2
    couplings = []
    for offset in corner_offsets:
        vector, length, weight = geometry(displacement, occupancy, offset)
        couplings.append(weight * exchange_scale * jnp.exp(-exchange_decay * (length - bond_length)))
    current = spin_vectors
    for update in range(15):
        sector = update if update < 8 else 14 - update
        sublattice = sector % 2
        quarter = sector // 2
        fraction = step_time if update == 7 else 0.5 * step_time
        torque = external
        for corner, offset in enumerate(corner_offsets):
            if sublattice == 0:
                torque = torque + couplings[corner][None] * roll_cells(current[1], offset, 1)
            else:
                torque = torque + roll_cells(couplings[corner][None] * current[0], offset, -1)
        chosen = current[sublattice]
        turned = rotate(chosen, torque, fraction)
        inside = (x_half == quarter % 2) & (y_half == quarter // 2)
        turned = jnp.where(inside[None], turned, chosen)
        current = current.at[sublattice].set(turned)
    first_density = jnp.zeros(spin_vectors.shape[2:], jnp.float32)
    second_density = jnp.zeros(spin_vectors.shape[2:], jnp.float32)
    for offset in corner_offsets:
        vector, length, weight = geometry(displacement, occupancy, offset)
        density = weight * jnp.exp(-density_decay * (length - bond_length))
        first_density = first_density + density
        second_density = second_density + roll_cells(density, offset, -1)
    first_slope = -0.5 / jnp.sqrt(1.0 + first_density)
    second_slope = -0.5 / jnp.sqrt(1.0 + second_density)
    first_force = jnp.zeros(spin_vectors.shape[1:], jnp.float32)
    second_force = jnp.zeros(spin_vectors.shape[1:], jnp.float32)
    for corner, offset in enumerate(corner_offsets):
        vector, length, weight = geometry(displacement, occupancy, offset)
        stretch = length - bond_length
        alignment = lax.optimization_barrier(jnp.sum(current[0] * roll_cells(current[1], offset, 1), axis=0))
        slopes = first_slope + roll_cells(second_slope, offset, 1)
        strength = -pair_decay * pair_scale * weight * jnp.exp(-pair_decay * stretch) - density_decay * weight * jnp.exp(-density_decay * stretch) * slopes + exchange_decay * couplings[corner] * alignment
        bond_force = strength[None] * vector / length[None]
        first_force = first_force + bond_force
        second_force = second_force - roll_cells(bond_force, offset, -1)
    return (current, jnp.stack([first_force, second_force]))
```

```python
import functools
import itertools

import jax
import jax.numpy as jnp
from jax import lax
from jax.experimental import pallas as pl
from jax.experimental.pallas import tpu as pltpu
from jax.sharding import PartitionSpec as P

step_time = 0.6
exchange_scale = 0.35
exchange_decay = 4.0
pair_scale = 0.5
pair_decay = 6.0
density_decay = 3.0
bond_length = 0.8660254037844386
corner_offsets = list(itertools.product((0, 1), repeat=3))
axes = ("gx", "gy", "gz")
MESH = pl.DeviceIdType.MESH

FIELDS = 14
STRIPS = 2


def working(rows, lanes):
    row = lax.broadcasted_iota(jnp.int32, (rows, lanes), 0)
    first, last = row % 4 == 0, row % 4 == 3

    def turn(v, n):
        return pltpu.roll(v, n % rows, 0)

    def below(pair, tile):
        a, b = pair
        if tile == 0:
            return jnp.where(first, turn(b, 5), turn(a, 1))
        return jnp.where(first, turn(a, 1), turn(b, 1))

    def above(pair, tile):
        a, b = pair
        if tile == 0:
            return jnp.where(last, turn(b, -1), turn(a, -1))
        return jnp.where(last, turn(a, 3), turn(b, -1))

    def z_below(v):
        return pltpu.roll(v, 1, 1)

    def z_above(v):
        return pltpu.roll(v, lanes - 1, 1)

    return below, above, z_below, z_above


def kernel(sizes, spin, disp, occ, field, out_s, out_f, E, PZ, RZ, SY, RY, W, WZ, J, J1, P3, RI, FS, FZ, ACC,
           send_sem, recv_sem):
    nx, ny, nz = sizes
    me = {a: lax.axis_index(a) for a in axes}
    count = dict(zip(axes, sizes))

    def peer(axis, step):
        n = count[axis]
        return {axis: lax.rem(me[axis] + (n + step), n)}

    peers = []
    for axis in axes:
        peers.append(peer(axis, 1))
        if count[axis] > 2:
            peers.append(peer(axis, -1))
    barrier = pltpu.get_barrier_semaphore()
    for p in peers:
        pl.semaphore_signal(barrier, inc=1, device_id=p, device_id_type=MESH)

    lane = lax.broadcasted_iota(jnp.int32, (8, 128), 1)
    row = lax.broadcasted_iota(jnp.int32, (8, 128), 0)
    upper = row < 4

    def swap(v):
        return pltpu.roll(v, 4, 0)

    def load_own(x, _):
        packed = [jnp.zeros((8, 128), jnp.float32)] * STRIPS
        for f in range(FIELDS):
            if f < 6:
                v = spin[f // 3, f % 3, x]
            elif f < 12:
                v = disp[(f - 6) // 3, f % 3, x]
            else:
                v = occ[f - 12, x].astype(jnp.float32)
            E[f, x, 0] = v
            g = f % 7
            moved = pltpu.roll(v, 8 + 16 * g, 1)
            packed[f // 7] = jnp.where(lane // 16 == g, moved, packed[f // 7])
        for s in range(STRIPS):
            PZ[s, x] = packed[s]
        return 0

    lax.fori_loop(0, 8, load_own, 0)

    def pack_rows(f, _):
        for x in range(4):
            a, b = E[f, x, 0], E[f, x + 4, 0]
            SY[0, f, x] = jnp.where(upper, a, swap(b))
            SY[1, f, x] = jnp.where(upper, swap(a), b)
        return 0

    lax.fori_loop(0, FIELDS, pack_rows, 0)
    pl.semaphore_wait(barrier, len(peers))

    def send(i, src, dst, to):
        c = pltpu.make_async_remote_copy(
            src_ref=src, dst_ref=dst, send_sem=send_sem.at[i], recv_sem=recv_sem.at[i],
            device_id=to, device_id_type=MESH)
        c.start()
        return c

    def exchange_x(i, lo, n, part, low, high):
        return [
            send(i, E.at[pl.ds(lo, n), pl.ds(0, low), part], E.at[pl.ds(lo, n), pl.ds(8, low), part], peer("gx", -1)),
            send(i + 1, E.at[pl.ds(lo, n), pl.ds(8 - high, high), part],
                 E.at[pl.ds(lo, n), pl.ds(16 - high, high), part], peer("gx", 1)),
        ]

    def exchange_y(i, lo, n):
        return [
            send(i, SY.at[0, pl.ds(lo, n)], RY.at[0, pl.ds(lo, n)], peer("gy", -1)),
            send(i + 1, SY.at[1, pl.ds(lo, n)], RY.at[1, pl.ds(lo, n)], peer("gy", 1)),
        ]

    zs = [send(0, PZ, RZ.at[0], peer("gz", -1))]
    if nz > 2:
        zs.append(send(1, PZ, RZ.at[1], peer("gz", 1)))
    ys = exchange_y(2, 0, FIELDS)
    xs = exchange_x(4, 0, FIELDS, 0, 4, 4)
    for c in zs:
        c.wait()
    for s in range(STRIPS):
        for x in range(8):
            v = RZ[0, s, x]
            if nz > 2:
                v = jnp.where(lane % 16 < 8, RZ[1, s, x], v)
            E[FIELDS + s, x, 0] = v
    lax.fori_loop(FIELDS, FIELDS + STRIPS, pack_rows, 0)
    ys2 = exchange_y(6, FIELDS, STRIPS)
    xs2 = exchange_x(8, FIELDS, STRIPS, 0, 4, 4)

    def unpack_rows(f, _):
        for x in range(4):
            lo, hi = RY[0, f, x], RY[1, f, x]
            E[f, x, 1] = jnp.where(upper, lo, swap(hi))
            E[f, x + 4, 1] = jnp.where(upper, swap(lo), hi)
        return 0

    for c in ys:
        c.wait()
    lax.fori_loop(0, FIELDS, unpack_rows, 0)
    xs3 = exchange_x(10, 0, FIELDS, 1, 2, 2)
    for c in ys2:
        c.wait()
    lax.fori_loop(FIELDS, FIELDS + STRIPS, unpack_rows, 0)
    xs4 = exchange_x(12, FIELDS, STRIPS, 1, 2, 2)
    for c in xs + xs2 + xs3 + xs4:
        c.wait()

    below, above, z_below, z_above = working(8, 256)

    def build(x, _):
        def tiles(f):
            t, g = E[f, x, 0], swap(E[f, x, 1])
            return jnp.where(upper, t, g), jnp.where(upper, g, t)

        strips = [tiles(FIELDS + s) for s in range(STRIPS)]
        for f in range(FIELDS):
            pair = tiles(f)
            for t in range(2):
                halo = pltpu.roll(strips[f // 7][t], 128 - 16 * (f % 7) - 8, 1)
                v = jnp.concatenate([pair[t], halo], axis=1)
                W[f, x, t] = v
                if f < 3:
                    WZ[f, x, t] = z_above(v)
                elif f < 6 or f in (9, 10, 11, 13):
                    WZ[f, x, t] = z_below(v)
        return 0

    lax.fori_loop(0, 16, build, 0)

    def before(x):
        return lax.rem(x + 15, 16)

    def after(x):
        return lax.rem(x + 1, 16)

    def pair_of(ref, f, x):
        return ref[f, x, 0], ref[f, x, 1]

    def partner(f, planes, o, tile):
        ref = WZ if o[2] else W
        if o[1]:
            return below(pair_of(ref, f, planes[o[0]]), tile)
        return ref[f, planes[o[0]], tile]

    def bonds(x, _):
        planes = (x, before(x))
        for t in range(2):
            own = [W[6 + k, x, t] for k in range(3)]
            here = W[12, x, t]
            for i, o in enumerate(corner_offsets):
                d = [(0.5 - o[k]) + (partner(9 + k, planes, o, t) - own[k]) for k in range(3)]
                w = here * partner(13, planes, o, t)
                r2 = d[0] * d[0] + d[1] * d[1] + d[2] * d[2]
                inverse = lax.rsqrt(r2)
                stretch = r2 * inverse - bond_length
                J[i, x, t] = w * exchange_scale * jnp.exp(-exchange_decay * stretch)
                P3[i, x, t] = w * jnp.exp(-density_decay * stretch)
                RI[i, x, t] = inverse
        return 0

    lax.fori_loop(0, 16, bonds, 0)

    def upper_bonds(x, _):
        planes = (x, after(x))
        for i, o in enumerate(corner_offsets):
            pair = pair_of(J, i, planes[o[0]])
            if o[2]:
                pair = [z_above(v) for v in pair]
            for t in range(2):
                J1[i, x, t] = above(pair, t) if o[1] else pair[t]
        return 0

    lax.fori_loop(0, 16, upper_bonds, 0)

    def update(u):
        sector = u if u < 8 else 14 - u
        sub, quarter = sector % 2, sector // 2
        half, tile = quarter % 2, quarter // 2
        scale = 0.5 * (step_time if u == 7 else 0.5 * step_time)
        source = 3 if sub == 0 else 0
        target = 3 * sub
        coupling = J if sub == 0 else J1

        def plane(x, _):
            planes = (x, before(x) if sub == 0 else after(x))
            h = [field[k] for k in range(3)]
            for k in range(3):
                total = None
                for ox in range(2):
                    for oz in range(2):
                        ref = WZ if oz else W
                        pair = pair_of(ref, source + k, planes[ox])
                        for oy in range(2):
                            i = 4 * ox + 2 * oy + oz
                            v = pair[tile] if oy == 0 else (below if sub == 0 else above)(pair, tile)
                            term = coupling[i, x, tile] * v
                            total = term if total is None else total + term
                h[k] = (h[k] + total) * scale
            s = [W[target + k, x, tile] for k in range(3)]

            def cross(a, b):
                return [a[1] * b[2] - a[2] * b[1], a[2] * b[0] - a[0] * b[2], a[0] * b[1] - a[1] * b[0]]

            once = cross(h, s)
            twice = cross(h, once)
            factor = 2.0 / (1.0 + (h[0] * h[0] + h[1] * h[1] + h[2] * h[2]))
            for k in range(3):
                v = s[k] + factor * (once[k] + twice[k])
                W[target + k, x, tile] = v
                WZ[target + k, x, tile] = z_above(v) if sub == 0 else z_below(v)
            return 0

        def pairs(m, _):
            base = 4 * half + 8 * m
            for n in range(4):
                plane(base + n, 0)
            return 0

        lax.fori_loop(0, 2, pairs, 0)

    for u in range(15):
        update(u)

    def slope(rho):
        return -0.5 * lax.rsqrt(1.0 + rho)

    def slopes(n, _):
        x = lax.rem(n + 15, 16)
        planes = (x, after(x))
        for t in range(2):
            FS[0, x, t] = slope(functools.reduce(jnp.add, [P3[i, x, t] for i in range(8)]))
        rows = []
        for oy in range(2):
            total = []
            for t in range(2):
                flat = P3[2 * oy, planes[0], t] + P3[4 + 2 * oy, planes[1], t]
                high = P3[2 * oy + 1, planes[0], t] + P3[5 + 2 * oy, planes[1], t]
                total.append(flat + z_above(high))
            rows.append(total)
        for t in range(2):
            v = slope(rows[0][t] + above(rows[1], t))
            FS[1, x, t] = v
            FZ[x, t] = z_below(v)
        return 0

    lax.fori_loop(0, 10, slopes, 0)

    def slope_partner(planes, o, tile):
        x = planes[o[0]]
        pair = (FZ[x, 0], FZ[x, 1]) if o[2] else (FS[1, x, 0], FS[1, x, 1])
        return below(pair, tile) if o[1] else pair[tile]

    def forces(x, _):
        planes = (x, before(x))
        sums = [[None] * 2 for _ in range(3)]
        parts = {}
        for t in range(2):
            own = [W[6 + k, x, t] for k in range(3)]
            spins = [W[k, x, t] for k in range(3)]
            mine = FS[0, x, t]
            for i, o in enumerate(corner_offsets):
                d = [(0.5 - o[k]) + (partner(9 + k, planes, o, t) - own[k]) for k in range(3)]
                align = functools.reduce(jnp.add, [spins[k] * partner(3 + k, planes, o, t) for k in range(3)])
                p = P3[i, x, t]
                g = (-pair_decay * pair_scale * (p * p) - density_decay * p * (mine + slope_partner(planes, o, t))
                     + exchange_decay * J[i, x, t] * align) * RI[i, x, t]
                for k in range(3):
                    v = g * d[k]
                    parts[i, t, k] = v
                    sums[k][t] = v if sums[k][t] is None else sums[k][t] + v
        for k in range(3):
            for t in range(2):
                ACC[k, x, t] = sums[k][t]
            for ox in range(2):
                rows = [[parts[4 * ox + 2 * oy, t, k] + z_above(parts[4 * ox + 2 * oy + 1, t, k]) for t in range(2)]
                        for oy in range(2)]
                for t in range(2):
                    v = rows[0][t] + above(rows[1], t)
                    if ox == 0:
                        ACC[3 + k, x, t] = -v
                    else:
                        ACC[3 + k, planes[1], t] = ACC[3 + k, planes[1], t] - v
        return 0

    lax.fori_loop(0, 9, forces, 0)

    def write(x, _):
        for f in range(6):
            for ref, out in ((W, out_s), (ACC, out_f)):
                a, b = ref[f, x, 0], ref[f, x, 1]
                out[f // 3, f % 3, x] = jnp.where(upper, a[:, :128], b[:, :128])
        return 0

    lax.fori_loop(0, 8, write, 0)


def on_device(sizes, spin_vectors, displacement, occupied, applied_field):
    vmem = pl.BlockSpec(memory_space=pltpu.VMEM)
    smem = pl.BlockSpec(memory_space=pltpu.SMEM)
    shape = jax.ShapeDtypeStruct(spin_vectors.shape, jnp.float32)

    def buffer(*lead):
        return pltpu.VMEM(lead + (8, 128), jnp.float32)

    def wide(*lead):
        return pltpu.VMEM(lead + (16, 2, 8, 256), jnp.float32)

    return pl.pallas_call(
        functools.partial(kernel, sizes),
        out_shape=(shape, shape),
        in_specs=[vmem, vmem, vmem, smem],
        out_specs=(vmem, vmem),
        scratch_shapes=[
            buffer(FIELDS + STRIPS, 16, 2),
            buffer(STRIPS, 8),
            buffer(2, STRIPS, 8),
            buffer(2, FIELDS + STRIPS, 4),
            buffer(2, FIELDS + STRIPS, 4),
            wide(FIELDS), wide(FIELDS), wide(8), wide(8), wide(8), wide(8), wide(2), wide(), wide(6),
            pltpu.SemaphoreType.DMA((14,)),
            pltpu.SemaphoreType.DMA((14,)),
        ],
        compiler_params=pltpu.CompilerParams(
            collective_id=0, has_side_effects=True, vmem_limit_bytes=60 * 1024 * 1024),
    )(spin_vectors, displacement, occupied, applied_field)


def solution(mesh):
    sizes = tuple(mesh.shape[a] for a in axes)
    block = P(None, None, "gx", "gy", "gz")
    return jax.shard_map(
        functools.partial(on_device, sizes),
        mesh=mesh,
        in_specs=(block, block, P(None, "gx", "gy", "gz"), P()),
        out_specs=(block, block),
        check_vma=False,
    )
```

```python
import functools
import itertools

import jax
import jax.numpy as jnp
from jax import lax
from jax.experimental import pallas as pl
from jax.experimental.pallas import tpu as pltpu
from jax.sharding import PartitionSpec as P

step_time = 0.6
exchange_scale = 0.35
exchange_decay = 4.0
pair_scale = 0.5
pair_decay = 6.0
density_decay = 3.0
bond_length = 0.8660254037844386
corner_offsets = list(itertools.product((0, 1), repeat=3))
axes = ("gx", "gy", "gz")
MESH = pl.DeviceIdType.MESH

FIELDS = 7
TO_BELOW = tuple(
    [(i // 4, i, 0, 2, 2 * (i % 4)) for i in range(8)] + [(2, 2 + i, 2, 2, 2 * i) for i in range(4)])
TO_ABOVE_0 = tuple([(0, i, 7, 1, i) for i in range(8)] + [(1, 2 + i, 5, 2, 2 * i) for i in range(4)])
TO_ABOVE_1 = tuple(
    [(i // 4, i, 6, 2, 2 * (i % 4)) for i in range(8)] + [(2, 2 + i, 4, 2, 2 * i) for i in range(4)])


@functools.cache
def turned_planes():
    need = {(0, x, y) for x in range(9) for y in range(9)} | {(1, x, y) for x in range(-1, 8) for y in range(-1, 8)}
    need |= {(b, x, y) for b in (0, 1) for x in range(8) for y in range(8)}
    planes = {}
    for u in reversed(range(15)):
        sector = u if u < 8 else 14 - u
        sub, quarter = sector % 2, sector // 2
        turned = [k for k in need if k[0] == sub and k[1] // 4 % 2 + 2 * (k[2] // 4 % 2) == quarter]
        planes[u] = sorted({k[1] for k in turned})
        for _, x, y in turned:
            for a, b, _ in corner_offsets:
                need.add((1, x - a, y - b) if sub == 0 else (0, x + a, y + b))
    return planes


def working(rows, lanes):
    row = lax.broadcasted_iota(jnp.int32, (rows, lanes), 0)
    first, last = row % 4 == 0, row % 4 == 3

    def turn(v, n):
        return pltpu.roll(v, n % rows, 0)

    def below(pair, tile):
        a, b = pair
        if tile == 0:
            return jnp.where(first, turn(b, 5), turn(a, 1))
        return jnp.where(first, turn(a, 1), turn(b, 1))

    def above(pair, tile):
        a, b = pair
        if tile == 0:
            return jnp.where(last, turn(b, -1), turn(a, -1))
        return jnp.where(last, turn(a, 3), turn(b, -1))

    def z_below(v):
        return pltpu.roll(v, 1, 1)

    def z_above(v):
        return pltpu.roll(v, lanes - 1, 1)

    return below, above, z_below, z_above


def kernel(sizes, spin, disp, occ, field, out_s, out_f, E, PZ, RZ, SU, RU, SD, RD, SX, RX, SC, RC, W, WZ, J, J1, P3, RI, FS, FZ, ACC,
           send_sem, recv_sem):
    nx, ny, nz = sizes
    me = {a: lax.axis_index(a) for a in axes}
    count = dict(zip(axes, sizes))

    def peer(axis, step):
        n = count[axis]
        return {axis: lax.rem(me[axis] + (n + step), n)}

    peers = []
    for axis in axes:
        peers.append(peer(axis, 1))
        if count[axis] > 2:
            peers.append(peer(axis, -1))
    barrier = pltpu.get_barrier_semaphore()
    for p in peers:
        pl.semaphore_signal(barrier, inc=1, device_id=p, device_id_type=MESH)

    lane = lax.broadcasted_iota(jnp.int32, (8, 128), 1)
    row = lax.broadcasted_iota(jnp.int32, (8, 128), 0)
    upper = row < 4

    def swap(v):
        return pltpu.roll(v, 4, 0)

    def load_own(x, _):
        for s in range(2):
            packed = jnp.zeros((8, 128), jnp.float32)
            for f in range(FIELDS):
                if f < 3:
                    v = spin[s, f, x]
                elif f < 6:
                    v = disp[s, f - 3, x]
                else:
                    v = occ[s, x].astype(jnp.float32)
                E[s, f, x, 0] = v
                packed = jnp.where(lane // 16 == f, pltpu.roll(v, 8 + 16 * f, 1), packed)
            PZ[s, x] = packed
        return 0

    lax.fori_loop(0, 8, load_own, 0)
    inner = (row >= 2) & (row < 6)

    def routes(s):
        return ((SU, RU, (0, 2)[s], (TO_ABOVE_0, TO_ABOVE_1)[s]), (SD, RD, 3 * s, TO_BELOW))

    def pack_rows(f, _):
        for s in range(2):
            own = [E[s, f, x, 0] for x in range(8)]
            for out, _unused, first, pieces in routes(s):
                tiles = {}
                for tile, x, low, n, to in pieces:
                    v = pltpu.roll(own[x], (to - low) % 8, 0)
                    tiles[tile] = jnp.where(row < to, tiles[tile], v) if to else v
                for tile, v in tiles.items():
                    out[f, first + tile] = v
            SX[0, s, f] = jnp.where(inner, own[2], swap(own[3]))
            SX[1, s, f] = jnp.where(inner, own[4], swap(own[5]))
        return 0

    def unpack_rows(f, _):
        for s in range(2):
            rows = [jnp.zeros((8, 128), jnp.float32)] * 8
            for _unused, arrived, first, pieces in routes(s):
                for tile, x, low, n, to in pieces:
                    v = pltpu.roll(arrived[f, first + tile], (low - to) % 8, 0)
                    rows[x] = jnp.where((row >= low) & (row < low + n), v, rows[x])
            for x in range(8):
                E[s, f, x, 1] = rows[x]
            SC[0, s, f] = jnp.where(inner, swap(rows[1]), rows[0])
            SC[1, s, f] = jnp.where(inner, swap(rows[7]), rows[6])
        return 0

    lax.fori_loop(0, FIELDS, pack_rows, 0)
    pl.semaphore_wait(barrier, len(peers))

    def send(i, src, dst, to):
        c = pltpu.make_async_remote_copy(
            src_ref=src, dst_ref=dst, send_sem=send_sem.at[i], recv_sem=recv_sem.at[i],
            device_id=to, device_id_type=MESH)
        c.start()
        return c

    def exchange_y(i, lo, n):
        return [
            send(i, SD.at[pl.ds(lo, n)], RD.at[pl.ds(lo, n)], peer("gy", -1)),
            send(i + 1, SU.at[pl.ds(lo, n)], RU.at[pl.ds(lo, n)], peer("gy", 1)),
        ]

    def exchange_x(i, lo, n):
        def plane(x):
            return E.at[:, pl.ds(lo, n), pl.ds(x, 2), 0]

        return [
            send(i, plane(0), plane(8), peer("gx", -1)),
            send(i + 1, plane(6), plane(14), peer("gx", 1)),
            send(i + 2, SX.at[0, :, pl.ds(lo, n)], RX.at[0, :, pl.ds(lo, n)], peer("gx", -1)),
            send(i + 3, SX.at[1, :, pl.ds(lo, n)], RX.at[1, :, pl.ds(lo, n)], peer("gx", 1)),
        ]

    zs = [send(0, PZ, RZ.at[0], peer("gz", -1))]
    if nz > 2:
        zs.append(send(1, PZ, RZ.at[1], peer("gz", 1)))
    ys = exchange_y(2, 0, FIELDS)
    xs = exchange_x(4, 0, FIELDS)
    for c in zs:
        c.wait()
    for s in range(2):
        for x in range(8):
            v = RZ[0, s, x]
            if nz > 2:
                v = jnp.where(lane % 16 < 8, RZ[1, s, x], v)
            E[s, FIELDS, x, 0] = v
    pack_rows(FIELDS, 0)
    ys += exchange_y(8, FIELDS, 1)
    xs += exchange_x(10, FIELDS, 1)
    for c in ys:
        c.wait()
    lax.fori_loop(0, FIELDS + 1, unpack_rows, 0)
    corners = [send(14 + i, SC.at[i], RC.at[i], peer("gx", 2 * i - 1)) for i in range(2)]

    below, above, z_below, z_above = working(8, 256)

    def build(x, _):
        def tiles(s, f):
            t, g = E[s, f, x, 0], swap(E[s, f, x, 1])
            return jnp.where(upper, t, g), jnp.where(upper, g, t)

        for s in range(2):
            strips = tiles(s, FIELDS)
            for f in range(FIELDS):
                pair = tiles(s, f)
                for t in range(2):
                    halo = pltpu.roll(strips[t], 128 - 16 * f - 8, 1)
                    v = jnp.concatenate([pair[t], halo], axis=1)
                    W[7 * s + f, x, t] = v
                    if s == 1:
                        WZ[7 + f, x, t] = z_below(v)
                    elif f < 3:
                        WZ[f, x, t] = z_above(v)
        return 0

    lax.fori_loop(0, 8, build, 0)
    for c in xs + corners:
        c.wait()

    def unpack_planes(f, _):
        for s in range(2):
            for i in range(2):
                v = RX[i, s, f]
                E[s, f, 10 + 2 * i, 0], E[s, f, 11 + 2 * i, 0] = v, swap(v)
                E[s, f, 10 + 2 * i, 1], E[s, f, 11 + 2 * i, 1] = v, v
                v = RC[i, s, f]
                E[s, f, 8 + 6 * i, 1], E[s, f, 9 + 6 * i, 1] = v, swap(v)
        return 0

    lax.fori_loop(0, FIELDS + 1, unpack_planes, 0)
    lax.fori_loop(8, 16, build, 0)

    def before(x):
        return lax.rem(x + 15, 16)

    def after(x):
        return lax.rem(x + 1, 16)

    def pair_of(ref, f, x):
        return ref[f, x, 0], ref[f, x, 1]

    def partner(f, planes, o, tile):
        ref = WZ if o[2] else W
        if o[1]:
            return below(pair_of(ref, f, planes[o[0]]), tile)
        return ref[f, planes[o[0]], tile]

    def bonds(x, _):
        planes = (x, before(x))
        for t in range(2):
            own = [W[3 + k, x, t] for k in range(3)]
            here = W[6, x, t]
            for i, o in enumerate(corner_offsets):
                d = [(0.5 - o[k]) + (partner(10 + k, planes, o, t) - own[k]) for k in range(3)]
                w = here * partner(13, planes, o, t)
                r2 = d[0] * d[0] + d[1] * d[1] + d[2] * d[2]
                inverse = lax.rsqrt(r2)
                stretch = r2 * inverse - bond_length
                J[i, x, t] = w * exchange_scale * jnp.exp(-exchange_decay * stretch)
                P3[i, x, t] = w * jnp.exp(-density_decay * stretch)
                RI[i, x, t] = inverse
        return 0

    lax.fori_loop(0, 16, bonds, 0)

    def upper_bonds(x, _):
        planes = (x, after(x))
        for i, o in enumerate(corner_offsets):
            pair = pair_of(J, i, planes[o[0]])
            if o[2]:
                pair = [z_above(v) for v in pair]
            for t in range(2):
                J1[i, x, t] = above(pair, t) if o[1] else pair[t]
        return 0

    lax.fori_loop(0, 16, upper_bonds, 0)

    def update(u):
        sector = u if u < 8 else 14 - u
        sub, quarter = sector % 2, sector // 2
        tile = quarter // 2
        scale = 0.5 * (step_time if u == 7 else 0.5 * step_time)
        source, target, step = (7, 0, -1) if sub == 0 else (0, 7, 1)
        coupling = J if sub == 0 else J1
        planes = turned_planes()[u]
        shift = below if sub == 0 else above

        @functools.cache
        def around(k, x):
            found = {}
            for oz in range(2):
                pair = pair_of(WZ if oz else W, source + k, x % 16)
                found[0, oz], found[1, oz] = pair[tile], shift(pair, tile)
            return found

        def cross(a, b):
            return [a[1] * b[2] - a[2] * b[1], a[2] * b[0] - a[0] * b[2], a[0] * b[1] - a[1] * b[0]]

        for x in planes:
            c = [coupling[i, x % 16, tile] for i in range(8)]
            h = []
            for k in range(3):
                total = field[k]
                for i, o in enumerate(corner_offsets):
                    total = total + c[i] * around(k, x + step * o[0])[o[1], o[2]]
                h.append(total * scale)
            s = [W[target + k, x % 16, tile] for k in range(3)]
            once = cross(h, s)
            twice = cross(h, once)
            factor = 2.0 / (1.0 + (h[0] * h[0] + h[1] * h[1] + h[2] * h[2]))
            for k in range(3):
                v = s[k] + factor * (once[k] + twice[k])
                W[target + k, x % 16, tile] = v
                WZ[target + k, x % 16, tile] = z_above(v) if sub == 0 else z_below(v)

    for u in range(15):
        update(u)

    def slope(rho):
        return -0.5 * lax.rsqrt(1.0 + rho)

    def slopes(n, _):
        x = lax.rem(n + 15, 16)
        planes = (x, after(x))
        for t in range(2):
            FS[0, x, t] = slope(functools.reduce(jnp.add, [P3[i, x, t] for i in range(8)]))
        rows = []
        for oy in range(2):
            total = []
            for t in range(2):
                flat = P3[2 * oy, planes[0], t] + P3[4 + 2 * oy, planes[1], t]
                high = P3[2 * oy + 1, planes[0], t] + P3[5 + 2 * oy, planes[1], t]
                total.append(flat + z_above(high))
            rows.append(total)
        for t in range(2):
            v = slope(rows[0][t] + above(rows[1], t))
            FS[1, x, t] = v
            FZ[x, t] = z_below(v)
        return 0

    lax.fori_loop(0, 10, slopes, 0)

    def slope_partner(planes, o, tile):
        x = planes[o[0]]
        pair = (FZ[x, 0], FZ[x, 1]) if o[2] else (FS[1, x, 0], FS[1, x, 1])
        return below(pair, tile) if o[1] else pair[tile]

    def forces(x, _):
        planes = (x, before(x))
        sums = [[None] * 2 for _ in range(3)]
        parts = {}
        for t in range(2):
            own = [W[3 + k, x, t] for k in range(3)]
            spins = [W[k, x, t] for k in range(3)]
            mine = FS[0, x, t]
            for i, o in enumerate(corner_offsets):
                d = [(0.5 - o[k]) + (partner(10 + k, planes, o, t) - own[k]) for k in range(3)]
                align = functools.reduce(jnp.add, [spins[k] * partner(7 + k, planes, o, t) for k in range(3)])
                p = P3[i, x, t]
                g = (-pair_decay * pair_scale * (p * p) - density_decay * p * (mine + slope_partner(planes, o, t))
                     + exchange_decay * J[i, x, t] * align) * RI[i, x, t]
                for k in range(3):
                    v = g * d[k]
                    parts[i, t, k] = v
                    sums[k][t] = v if sums[k][t] is None else sums[k][t] + v
        for k in range(3):
            for t in range(2):
                ACC[k, x, t] = sums[k][t]
            for ox in range(2):
                rows = [[parts[4 * ox + 2 * oy, t, k] + z_above(parts[4 * ox + 2 * oy + 1, t, k]) for t in range(2)]
                        for oy in range(2)]
                for t in range(2):
                    v = rows[0][t] + above(rows[1], t)
                    if ox == 0:
                        ACC[3 + k, x, t] = -v
                    else:
                        ACC[3 + k, planes[1], t] = ACC[3 + k, planes[1], t] - v
        return 0

    lax.fori_loop(0, 9, forces, 0)

    def write(x, _):
        for f in range(6):
            for ref, at, out in ((W, 7 * (f // 3) + f % 3, out_s), (ACC, f, out_f)):
                a, b = ref[at, x, 0], ref[at, x, 1]
                out[f // 3, f % 3, x] = jnp.where(upper, a[:, :128], b[:, :128])
        return 0

    lax.fori_loop(0, 8, write, 0)


def on_device(sizes, spin_vectors, displacement, occupied, applied_field):
    vmem = pl.BlockSpec(memory_space=pltpu.VMEM)
    smem = pl.BlockSpec(memory_space=pltpu.SMEM)
    shape = jax.ShapeDtypeStruct(spin_vectors.shape, jnp.float32)

    def buffer(*lead):
        return pltpu.VMEM(lead + (8, 128), jnp.float32)

    def wide(*lead):
        return pltpu.VMEM(lead + (16, 2, 8, 256), jnp.float32)

    return pl.pallas_call(
        functools.partial(kernel, sizes),
        out_shape=(shape, shape),
        in_specs=[vmem, vmem, vmem, smem],
        out_specs=(vmem, vmem),
        scratch_shapes=[
            buffer(2, FIELDS + 1, 16, 2),
            buffer(2, 8), buffer(2, 2, 8),
            buffer(FIELDS + 1, 5), buffer(FIELDS + 1, 5),
            buffer(FIELDS + 1, 6), buffer(FIELDS + 1, 6),
            buffer(2, 2, FIELDS + 1), buffer(2, 2, FIELDS + 1),
            buffer(2, 2, FIELDS + 1), buffer(2, 2, FIELDS + 1),
            wide(14), wide(14), wide(8), wide(8), wide(8), wide(8), wide(2), wide(), wide(6),
            pltpu.SemaphoreType.DMA((16,)),
            pltpu.SemaphoreType.DMA((16,)),
        ],
        compiler_params=pltpu.CompilerParams(
            collective_id=0, has_side_effects=True, vmem_limit_bytes=60 * 1024 * 1024),
    )(spin_vectors, displacement, occupied, applied_field)


def solution(mesh):
    sizes = tuple(mesh.shape[a] for a in axes)
    block = P(None, None, "gx", "gy", "gz")
    return jax.shard_map(
        functools.partial(on_device, sizes),
        mesh=mesh,
        in_specs=(block, block, P(None, "gx", "gy", "gz"), P()),
        out_specs=(block, block),
        check_vma=False,
    )
```

```python
import functools
import itertools

import jax
import jax.numpy as jnp
from jax import lax
from jax.experimental import pallas as pl
from jax.experimental.pallas import tpu as pltpu
from jax.sharding import PartitionSpec as P

step_time = 0.6
exchange_scale = 0.35
exchange_decay = 4.0
pair_scale = 0.5
pair_decay = 6.0
density_decay = 3.0
bond_length = 0.8660254037844386
corner_offsets = list(itertools.product((0, 1), repeat=3))
axes = ("gx", "gy", "gz")
MESH = pl.DeviceIdType.MESH

DISPLACED, SPUN = 0, 1
GROUPS = ((0, 4), (9, 3))
ARRAYS = 16


def fields_of(group):
    first, n = GROUPS[group]
    return [(first + n * s + f, 7 * s + f + (3 if group == DISPLACED else 0), s) for s in range(2) for f in range(n)]


def strip_of(group):
    first, n = GROUPS[group]
    return first + 2 * n


TO_BELOW = tuple(
    [(i // 4, i, 0, 2, 2 * (i % 4)) for i in range(8)] + [(2, 2 + i, 2, 2, 2 * i) for i in range(4)])
TO_ABOVE_0 = tuple([(0, i, 7, 1, i) for i in range(8)] + [(1, 2 + i, 5, 2, 2 * i) for i in range(4)])
TO_ABOVE_1 = tuple(
    [(i // 4, i, 6, 2, 2 * (i % 4)) for i in range(8)] + [(2, 2 + i, 4, 2, 2 * i) for i in range(4)])


@functools.cache
def turned_planes():
    need = {(0, x, y) for x in range(9) for y in range(9)} | {(1, x, y) for x in range(-1, 8) for y in range(-1, 8)}
    need |= {(b, x, y) for b in (0, 1) for x in range(8) for y in range(8)}
    planes = {}
    for u in reversed(range(15)):
        sector = u if u < 8 else 14 - u
        sub, quarter = sector % 2, sector // 2
        turned = [k for k in need if k[0] == sub and k[1] // 4 % 2 + 2 * (k[2] // 4 % 2) == quarter]
        planes[u] = sorted({k[1] for k in turned})
        for _, x, y in turned:
            for a, b, _ in corner_offsets:
                need.add((1, x - a, y - b) if sub == 0 else (0, x + a, y + b))
    return planes


def working(rows, lanes):
    row = lax.broadcasted_iota(jnp.int32, (rows, lanes), 0)
    first, last = row % 4 == 0, row % 4 == 3

    def turn(v, n):
        return pltpu.roll(v, n % rows, 0)

    def below(pair, tile):
        a, b = pair
        if tile == 0:
            return jnp.where(first, turn(b, 5), turn(a, 1))
        return jnp.where(first, turn(a, 1), turn(b, 1))

    def above(pair, tile):
        a, b = pair
        if tile == 0:
            return jnp.where(last, turn(b, -1), turn(a, -1))
        return jnp.where(last, turn(a, 3), turn(b, -1))

    def z_below(v):
        return pltpu.roll(v, 1, 1)

    def z_above(v):
        return pltpu.roll(v, lanes - 1, 1)

    return below, above, z_below, z_above


def place_rows():
    up, down, at, n_up, n_down = [], [], [], 0, 0
    for group in (DISPLACED, SPUN):
        for s in [s for _, _, s in fields_of(group)] + [1]:
            up.append(n_up)
            down.append(n_down)
            at.append(s)
            n_up += 2 + s
            n_down += 3
    return up + [n_up], down + [n_down], at


UP, DOWN, GEOMETRY = place_rows()


def kernel(sizes, spin, disp, occ, field, out_s, out_f, E, PZ, RZ, SU, RU, SD, RD, SX, RX, SC, RC, W, WZ, J, J1, P3, RI, FS, FZ, ACC,
           send_sem, recv_sem):
    nx, ny, nz = sizes
    me = {a: lax.axis_index(a) for a in axes}
    count = dict(zip(axes, sizes))

    def peer(axis, step):
        n = count[axis]
        return {axis: lax.rem(me[axis] + (n + step), n)}

    peers = []
    for axis in axes:
        peers.append(peer(axis, 1))
        if count[axis] > 2:
            peers.append(peer(axis, -1))
    barrier = pltpu.get_barrier_semaphore()
    for p in peers:
        pl.semaphore_signal(barrier, inc=1, device_id=p, device_id_type=MESH)

    lane = lax.broadcasted_iota(jnp.int32, (8, 128), 1)
    row = lax.broadcasted_iota(jnp.int32, (8, 128), 0)
    upper = row < 4

    def swap(v):
        return pltpu.roll(v, 4, 0)

    def load_own(x, _):
        for group in (DISPLACED, SPUN):
            packed = jnp.zeros((8, 128), jnp.float32)
            for n, (e, w, s) in enumerate(fields_of(group)):
                f = w % 7
                if f < 3:
                    v = spin[s, f, x]
                elif f < 6:
                    v = disp[s, f - 3, x]
                else:
                    v = occ[s, x].astype(jnp.float32)
                E[e, x, 0] = v
                packed = jnp.where(lane // 16 == n, pltpu.roll(v, (8 + 16 * n) % 128, 1), packed)
            PZ[group, x] = packed
        return 0

    lax.fori_loop(0, 8, load_own, 0, unroll=2)
    inner = (row >= 2) & (row < 6)

    def routes(e):
        return ((SU, RU, UP[e], (TO_ABOVE_0, TO_ABOVE_1)[GEOMETRY[e]]), (SD, RD, DOWN[e], TO_BELOW))

    def pack_rows(e):
        own = [E[e, x, 0] for x in range(8)]
        for out, _unused, first, pieces in routes(e):
            tiles = {}
            for tile, x, low, n, to in pieces:
                v = pltpu.roll(own[x], (to - low) % 8, 0)
                tiles[tile] = jnp.where(row < to, tiles[tile], v) if to else v
            for tile, v in tiles.items():
                out[first + tile] = v
        SX[0, e] = jnp.where(inner, own[2], swap(own[3]))
        SX[1, e] = jnp.where(inner, own[4], swap(own[5]))

    def unpack_rows(e):
        rows = [jnp.zeros((8, 128), jnp.float32)] * 8
        for _unused, arrived, first, pieces in routes(e):
            for tile, x, low, n, to in pieces:
                v = pltpu.roll(arrived[first + tile], (low - to) % 8, 0)
                rows[x] = jnp.where((row >= low) & (row < low + n), v, rows[x])
        for x in range(8):
            E[e, x, 1] = rows[x]
        SC[0, e] = jnp.where(inner, swap(rows[1]), rows[0])
        SC[1, e] = jnp.where(inner, swap(rows[7]), rows[6])

    def arrays_of(group):
        return range(GROUPS[group][0], strip_of(group) + 1)

    for group in (DISPLACED, SPUN):
        for e, _, _ in fields_of(group):
            pack_rows(e)
    pl.semaphore_wait(barrier, len(peers))

    def send(i, src, dst, to):
        c = pltpu.make_async_remote_copy(
            src_ref=src, dst_ref=dst, send_sem=send_sem.at[i], recv_sem=recv_sem.at[i],
            device_id=to, device_id_type=MESH)
        c.start()
        return c

    def exchange_y(i, lo, hi):
        up = pl.ds(UP[lo], UP[hi] - UP[lo])
        down = pl.ds(DOWN[lo], DOWN[hi] - DOWN[lo])
        return [
            send(i, SD.at[down], RD.at[down], peer("gy", -1)),
            send(i + 1, SU.at[up], RU.at[up], peer("gy", 1)),
        ]

    def exchange_x(i, lo, hi):
        part = pl.ds(lo, hi - lo)

        def plane(x):
            return E.at[part, pl.ds(x, 2), 0]

        return [
            send(i, plane(0), plane(8), peer("gx", -1)),
            send(i + 1, plane(6), plane(14), peer("gx", 1)),
            send(i + 2, SX.at[0, part], RX.at[0, part], peer("gx", -1)),
            send(i + 3, SX.at[1, part], RX.at[1, part], peer("gx", 1)),
        ]

    def exchange_z(i, group):
        found = [send(i, PZ.at[group], RZ.at[0, group], peer("gz", -1))]
        if nz > 2:
            found.append(send(i + 1, PZ.at[group], RZ.at[1, group], peer("gz", 1)))
        return found

    def take_strips(group, copies):
        for c in copies:
            c.wait()
        for x in range(8):
            v = RZ[0, group, x]
            if nz > 2:
                v = jnp.where(lane % 16 < 8, RZ[1, group, x], v)
            E[strip_of(group), x, 0] = v
        pack_rows(strip_of(group))

    def corner_copies(i, group):
        part = pl.ds(GROUPS[group][0], len(arrays_of(group)))
        return [send(i + n, SC.at[n, part], RC.at[n, part], peer("gx", 2 * n - 1)) for n in range(2)]

    z0 = exchange_z(0, DISPLACED)
    ys0 = exchange_y(4, GROUPS[0][0], strip_of(0))
    xs0 = exchange_x(12, GROUPS[0][0], strip_of(0))
    z1 = exchange_z(2, SPUN)
    take_strips(DISPLACED, z0)
    ys0 += exchange_y(6, strip_of(0), strip_of(0) + 1)
    ys1 = exchange_y(8, GROUPS[1][0], strip_of(1))
    xs0 += exchange_x(16, strip_of(0), strip_of(0) + 1)
    xs1 = exchange_x(20, GROUPS[1][0], strip_of(1))
    take_strips(SPUN, z1)
    ys1 += exchange_y(10, strip_of(1), strip_of(1) + 1)
    xs1 += exchange_x(24, strip_of(1), strip_of(1) + 1)
    for c in ys0:
        c.wait()
    for e in arrays_of(DISPLACED):
        unpack_rows(e)
    corners0 = corner_copies(28, DISPLACED)

    below, above, z_below, z_above = working(8, 256)

    def build(group, x, _):
        def tiles(e):
            t, g = E[e, x, 0], swap(E[e, x, 1])
            return jnp.where(upper, t, g), jnp.where(upper, g, t)

        strips = tiles(strip_of(group))
        for n, (e, w, s) in enumerate(fields_of(group)):
            pair = tiles(e)
            for t in range(2):
                halo = pltpu.roll(strips[t], (128 - 16 * n - 8) % 128, 1)
                v = jnp.concatenate([pair[t], halo], axis=1)
                W[w, x, t] = v
                if s == 1:
                    WZ[w, x, t] = z_below(v)
                elif group == SPUN:
                    WZ[w, x, t] = z_above(v)
        return 0

    build0 = functools.partial(build, DISPLACED)
    build1 = functools.partial(build, SPUN)

    def unpack_planes(group):
        for e in arrays_of(group):
            for i in range(2):
                v = RX[i, e]
                E[e, 10 + 2 * i, 0], E[e, 11 + 2 * i, 0] = v, swap(v)
                E[e, 10 + 2 * i, 1], E[e, 11 + 2 * i, 1] = v, v
                v = RC[i, e]
                E[e, 8 + 6 * i, 1], E[e, 9 + 6 * i, 1] = v, swap(v)

    def before(x):
        return lax.rem(x + 15, 16)

    def after(x):
        return lax.rem(x + 1, 16)

    def pair_of(ref, f, x):
        return ref[f, x, 0], ref[f, x, 1]

    def partner(f, planes, o, tile):
        ref = WZ if o[2] else W
        if o[1]:
            return below(pair_of(ref, f, planes[o[0]]), tile)
        return ref[f, planes[o[0]], tile]

    def bonds(x, _):
        planes = (x, before(x))
        for t in range(2):
            own = [W[3 + k, x, t] for k in range(3)]
            here = W[6, x, t]
            for i, o in enumerate(corner_offsets):
                d = [(0.5 - o[k]) + (partner(10 + k, planes, o, t) - own[k]) for k in range(3)]
                w = here * partner(13, planes, o, t)
                r2 = d[0] * d[0] + d[1] * d[1] + d[2] * d[2]
                inverse = lax.rsqrt(r2)
                stretch = r2 * inverse - bond_length
                J[i, x, t] = w * exchange_scale * jnp.exp(-exchange_decay * stretch)
                P3[i, x, t] = w * jnp.exp(-density_decay * stretch)
                RI[i, x, t] = inverse
        return 0

    lax.fori_loop(0, 8, build0, 0, unroll=2)
    lax.fori_loop(1, 8, bonds, 0)
    for c in xs0 + corners0:
        c.wait()
    unpack_planes(DISPLACED)
    lax.fori_loop(8, 16, build0, 0, unroll=2)
    for c in ys1:
        c.wait()
    for e in arrays_of(SPUN):
        unpack_rows(e)
    corners1 = corner_copies(30, SPUN)
    bonds(0, 0)
    lax.fori_loop(8, 12, bonds, 0)
    lax.fori_loop(13, 16, bonds, 0)

    def upper_bonds(x, _):
        planes = (x, after(x))
        for i, o in enumerate(corner_offsets):
            pair = pair_of(J, i, planes[o[0]])
            if o[2]:
                pair = [z_above(v) for v in pair]
            for t in range(2):
                J1[i, x, t] = above(pair, t) if o[1] else pair[t]
        return 0

    lax.fori_loop(0, 16, upper_bonds, 0, unroll=4)

    lax.fori_loop(0, 8, build1, 0, unroll=2)
    for c in xs1 + corners1:
        c.wait()
    unpack_planes(SPUN)
    lax.fori_loop(8, 16, build1, 0, unroll=2)

    def update(u):
        sector = u if u < 8 else 14 - u
        sub, quarter = sector % 2, sector // 2
        tile = quarter // 2
        scale = 0.5 * (step_time if u == 7 else 0.5 * step_time)
        source, target, step = (7, 0, -1) if sub == 0 else (0, 7, 1)
        coupling = J if sub == 0 else J1
        planes = turned_planes()[u]
        shift = below if sub == 0 else above

        @functools.cache
        def around(k, x):
            found = {}
            for oz in range(2):
                pair = pair_of(WZ if oz else W, source + k, x % 16)
                found[0, oz], found[1, oz] = pair[tile], shift(pair, tile)
            return found

        def cross(a, b):
            return [a[1] * b[2] - a[2] * b[1], a[2] * b[0] - a[0] * b[2], a[0] * b[1] - a[1] * b[0]]

        for x in planes:
            c = [coupling[i, x % 16, tile] for i in range(8)]
            h = []
            for k in range(3):
                total = field[k]
                for i, o in enumerate(corner_offsets):
                    total = total + c[i] * around(k, x + step * o[0])[o[1], o[2]]
                h.append(total * scale)
            s = [W[target + k, x % 16, tile] for k in range(3)]
            once = cross(h, s)
            twice = cross(h, once)
            factor = 2.0 / (1.0 + (h[0] * h[0] + h[1] * h[1] + h[2] * h[2]))
            for k in range(3):
                v = s[k] + factor * (once[k] + twice[k])
                W[target + k, x % 16, tile] = v
                WZ[target + k, x % 16, tile] = z_above(v) if sub == 0 else z_below(v)

    for u in range(15):
        update(u)

    def slope(rho):
        return -0.5 * lax.rsqrt(1.0 + rho)

    def slopes(n, _):
        x = lax.rem(n + 15, 16)
        planes = (x, after(x))
        for t in range(2):
            FS[0, x, t] = slope(functools.reduce(jnp.add, [P3[i, x, t] for i in range(8)]))
        rows = []
        for oy in range(2):
            total = []
            for t in range(2):
                flat = P3[2 * oy, planes[0], t] + P3[4 + 2 * oy, planes[1], t]
                high = P3[2 * oy + 1, planes[0], t] + P3[5 + 2 * oy, planes[1], t]
                total.append(flat + z_above(high))
            rows.append(total)
        for t in range(2):
            v = slope(rows[0][t] + above(rows[1], t))
            FS[1, x, t] = v
            FZ[x, t] = z_below(v)
        return 0

    lax.fori_loop(0, 10, slopes, 0, unroll=5)

    def slope_partner(planes, o, tile):
        x = planes[o[0]]
        pair = (FZ[x, 0], FZ[x, 1]) if o[2] else (FS[1, x, 0], FS[1, x, 1])
        return below(pair, tile) if o[1] else pair[tile]

    def forces(x, _):
        planes = (x, before(x))
        sums = [[None] * 2 for _ in range(3)]
        parts = {}
        for t in range(2):
            own = [W[3 + k, x, t] for k in range(3)]
            spins = [W[k, x, t] for k in range(3)]
            mine = FS[0, x, t]
            for i, o in enumerate(corner_offsets):
                d = [(0.5 - o[k]) + (partner(10 + k, planes, o, t) - own[k]) for k in range(3)]
                align = functools.reduce(jnp.add, [spins[k] * partner(7 + k, planes, o, t) for k in range(3)])
                p = P3[i, x, t]
                g = (-pair_decay * pair_scale * (p * p) - density_decay * p * (mine + slope_partner(planes, o, t))
                     + exchange_decay * J[i, x, t] * align) * RI[i, x, t]
                for k in range(3):
                    v = g * d[k]
                    parts[i, t, k] = v
                    sums[k][t] = v if sums[k][t] is None else sums[k][t] + v
        for k in range(3):
            for t in range(2):
                ACC[k, x, t] = sums[k][t]
            for ox in range(2):
                rows = [[parts[4 * ox + 2 * oy, t, k] + z_above(parts[4 * ox + 2 * oy + 1, t, k]) for t in range(2)]
                        for oy in range(2)]
                for t in range(2):
                    v = rows[0][t] + above(rows[1], t)
                    if ox == 0:
                        ACC[3 + k, x, t] = -v
                    else:
                        ACC[3 + k, planes[1], t] = ACC[3 + k, planes[1], t] - v
        return 0

    lax.fori_loop(0, 9, forces, 0)

    def write(x, _):
        for f in range(6):
            for ref, at, out in ((W, 7 * (f // 3) + f % 3, out_s), (ACC, f, out_f)):
                a, b = ref[at, x, 0], ref[at, x, 1]
                out[f // 3, f % 3, x] = jnp.where(upper, a[:, :128], b[:, :128])
        return 0

    lax.fori_loop(0, 8, write, 0, unroll=4)


def on_device(sizes, spin_vectors, displacement, occupied, applied_field):
    vmem = pl.BlockSpec(memory_space=pltpu.VMEM)
    smem = pl.BlockSpec(memory_space=pltpu.SMEM)
    shape = jax.ShapeDtypeStruct(spin_vectors.shape, jnp.float32)

    def buffer(*lead):
        return pltpu.VMEM(lead + (8, 128), jnp.float32)

    def wide(*lead):
        return pltpu.VMEM(lead + (16, 2, 8, 256), jnp.float32)

    return pl.pallas_call(
        functools.partial(kernel, sizes),
        out_shape=(shape, shape),
        in_specs=[vmem, vmem, vmem, smem],
        out_specs=(vmem, vmem),
        scratch_shapes=[
            buffer(ARRAYS, 16, 2),
            buffer(2, 8), buffer(2, 2, 8),
            buffer(UP[-1]), buffer(UP[-1]),
            buffer(DOWN[-1]), buffer(DOWN[-1]),
            buffer(2, ARRAYS), buffer(2, ARRAYS),
            buffer(2, ARRAYS), buffer(2, ARRAYS),
            wide(14), wide(14), wide(8), wide(8), wide(8), wide(8), wide(2), wide(), wide(6),
            pltpu.SemaphoreType.DMA((32,)),
            pltpu.SemaphoreType.DMA((32,)),
        ],
        compiler_params=pltpu.CompilerParams(
            collective_id=0, has_side_effects=True, vmem_limit_bytes=60 * 1024 * 1024),
    )(spin_vectors, displacement, occupied, applied_field)


def solution(mesh):
    sizes = tuple(mesh.shape[a] for a in axes)
    block = P(None, None, "gx", "gy", "gz")
    return jax.shard_map(
        functools.partial(on_device, sizes),
        mesh=mesh,
        in_specs=(block, block, P(None, "gx", "gy", "gz"), P()),
        out_specs=(block, block),
        check_vma=False,
    )
```
